256 devices in a mesh: slab: 64 (over y, z, core), tile: 4 (over x).
Axes of the slice: x: 4, y: 4, z: 8, core: 2. Of those that a mesh axis runs over, the one named last changes fastest.
Arguments:
- grid: bfloat16 [512, 256, 1024], P('slab', 'tile'), may hold values from -6 to 6
- type_table: float32 [16, 8], replicated, may hold values from -4 to 4
- counts: int32 [4096], P(('slab', 'tile')), may hold values from 10 to 120
- types: int32 [4096, 128], P(('slab', 'tile')), may hold values from 0 to 15
- offsets: float32 [4096, 3, 128], P(('slab', 'tile')), may hold values from 0 to 0.999
- route: int32 [4096, 1], P('slab'), may hold values from 0 to 63; in each aligned block of 64 rows (0 to 63, 64 to 127, ...) at most 2 rows name the same one
- base_y: int32 [4096], P(('slab', 'tile')), may hold values from 0 to 223
- base_z: int32 [4096], P(('slab', 'tile')), may hold values from 0 to 95
Outputs:
- energy: float32 [4096], P(('slab', 'tile'))
The draws below stay inside these ranges and needn't reach their ends.
Inputs may be any that keep to these rules, and one draw needn't show every extreme that they name: `route`: among the rows of one aligned block of 64 poses (those starting on one group of tile devices), at most 2 name the same slab.
All inputs are finite; a program needn't handle non-finite values.
Results may differ from the reference program's by a relative error of at most 0.0003.
Values may be sent and summed in bfloat16 or wider, within the bound.
No kernel may reach another device: no remote copies, remote signals or barrier semaphores. Data moves between devices by JAX's collectives and lax.ppermute only.
A program may use at most 64 MiB of HBM per device.

```python
import math
import jax
import jax.numpy as jnp
import numpy as np

CH = 8
TYPES = 16
ATOMS = 128
SPAN = 32
CX = 8
NZ = 128
POSE_DEV = 16
NX = 512
NY = 256
POSES = 4096
SLOT_CAP = 2
N_SLAB = 64


def plant(drawn, own_key, least, top_value):
    extent = drawn.shape
    place = [jax.random.randint(jax.random.fold_in(own_key, axis), (), 0, extent[axis]) for axis in range(len(extent))]
    drawn = drawn.at[tuple(place)].set(least)
    longest = extent.index(max(extent))
    place[longest] = (place[longest] + 1) % extent[longest]
    return drawn.at[tuple(place)].set(top_value)


def steps_of(own_key, extent, pieces, low, top_value):
    level, own = 1.0, jax.random.fold_in(own_key, 6)
    for axis_at, parts in pieces:
        heights = jnp.exp(jax.random.uniform(jax.random.fold_in(own, axis_at), (parts,), jnp.float32, low / len(pieces), top_value / len(pieces)))
        level = level * jnp.repeat(heights, extent[axis_at] // parts).reshape([-1 if axis == axis_at else 1 for axis in range(len(extent))])
    return level


def assign_block(key, own, number, rows, number_of, top, bound, slope):
    ranking = jax.random.permutation(key, number_of)
    crowded, common = portions_of(number_of, rows * top, bound, slope, True), portions_of(number_of, rows * top, bound, slope, False)
    places = jnp.arange(number_of)

    def named(tallies, turn):
        used = int((tallies > 0).sum())
        fixed = max(1, used // 4)
        moved = fixed + (places - fixed + turn * (used - fixed)) % max(1, number_of - fixed)
        return jnp.zeros((number_of,), jnp.int32).at[ranking[jnp.where(places < fixed, places, moved)]].set(jnp.asarray(tallies, jnp.int32))

    tallies = jnp.where(number % 4 == 0, named(crowded, number // 4), named(common, number - number // 4 - 1))
    mixed = jax.random.permutation(jax.random.fold_in(own, 3), number_of)
    giver, taker = mixed[0:number_of // 2 * 2:2], mixed[1:number_of // 2 * 2:2]
    margin = jnp.minimum(tallies[giver] - 1, bound - tallies[taker]) // 2
    margin = jnp.where((giver == ranking[0]) | (taker == ranking[0]) | (tallies[taker] == 0), 0, jnp.maximum(margin, 0))
    moved = jax.random.randint(jax.random.fold_in(own, 4), (number_of // 2,), 0, 1 << 20) % (margin + 1)
    tallies = tallies.at[giver].add(-moved).at[taker].add(moved)
    members = jnp.searchsorted(jnp.cumsum(tallies), jnp.arange(rows * top), side="right").astype(jnp.int32)
    table = members.reshape(top, rows).T
    table = table[jax.random.permutation(jax.random.fold_in(own, 1), rows)]
    turn = jax.random.randint(jax.random.fold_in(own, 2), (rows, 1), 0, top)
    return jnp.take_along_axis(table, (jnp.arange(top)[None, :] + turn) % top, axis=1)


def portions_of(count, total, reach, skew, full):
    weights = [(1 << 20) // math.isqrt(grade ** skew) + 1 for grade in range(1, count + 1)]
    largest = reach if full else min(reach, max(-(-total // count), total * weights[0] // sum(weights)))
    least = 1 if total - largest >= count - 1 else 0
    holding, spare = [largest] + [least] * (count - 1), total - largest - least * (count - 1)
    while spare > 0:
        free = [i for i in range(1, count) if holding[i] < largest] or [i for i in range(1, count) if holding[i] < reach]
        mass, remaining = sum([weights[i] for i in free]), spare
        for i in free:
            extra = min(reach - holding[i], max(1, remaining * weights[i] // mass), spare)
            holding[i] = holding[i] + extra
            spare = spare - extra
    return np.array(holding)


def scatter_about(stream_key, dims, spread, reach, split=(), dtype=jnp.bfloat16):
    values = jax.random.normal(stream_key, dims, jnp.float32) * spread
    if len(split) > 0:
        values = steps_of(stream_key, dims, split, -0.22, 0.18) * values
    return jnp.clip(values, min=-reach, max=reach).astype(dtype)


def setup_inputs(seed: int = 0) -> dict:
    splits = jax.random.split(jax.random.key(seed), 9)
    grid = scatter_about(splits[0], (NX, NY, NZ * CH), 1.0, 6.0, ((0, 64), (1, 4)))
    type_table = scatter_about(splits[1], (TYPES, CH), 1.0, 4.0, (), jnp.float32)
    counts = plant(jax.random.randint(splits[2], (POSES,), 10, 121), jax.random.fold_in(splits[2], 1), 10, 120).astype(jnp.int32)
    types = plant(jax.random.randint(splits[3], (POSES, ATOMS), 0, TYPES), jax.random.fold_in(splits[3], 1), 0, TYPES - 1).astype(jnp.int32)
    offsets = jnp.clip(0.999 * jax.random.uniform(splits[4], (POSES, 3, ATOMS), jnp.float32) ** steps_of(splits[4], (POSES, 3, ATOMS), ((0, 256),), -0.2, 0.2), 0.0, 0.999)
    route_keys = jax.random.split(jax.random.fold_in(splits[5], 1), POSES // (4 * POSE_DEV))
    route_turns = jax.random.permutation(jax.random.fold_in(splits[5], 3), POSES // (4 * POSE_DEV))
    route = jax.vmap(lambda own, number: assign_block(jax.random.fold_in(splits[5], 2), own, number, 4 * POSE_DEV, N_SLAB, 1, SLOT_CAP, 2))(route_keys, route_turns).reshape((POSES, 1))
    base_y = plant(jax.random.randint(splits[6], (POSES,), 0, NY - SPAN), jax.random.fold_in(splits[6], 1), 0, (NY - SPAN) - 1).astype(jnp.int32)
    base_z = plant(jax.random.randint(splits[7], (POSES,), 0, NZ - SPAN), jax.random.fold_in(splits[7], 1), 0, (NZ - SPAN) - 1).astype(jnp.int32)
    return {"grid": grid, "type_table": type_table, "counts": counts, "types": types, "offsets": offsets, "route": route, "base_y": base_y, "base_z": base_z}


def reference(grid, type_table, counts, types, offsets, route, base_y, base_z):
    local_x = offsets[:, 0, :] * (CX - 1)
    pos_y = base_y[:, None].astype(jnp.float32) + offsets[:, 1, :] * SPAN
    pos_z = base_z[:, None].astype(jnp.float32) + offsets[:, 2, :] * SPAN
    live = (jnp.arange(ATOMS)[None, :] < counts[:, None]).astype(jnp.float32) / counts[:, None].astype(jnp.float32)
    weights = type_table[types] * live[:, :, None]
    floor_x = jnp.floor(local_x)
    floor_y = jnp.floor(pos_y)
    floor_z = jnp.floor(pos_z)
    frac_x = local_x - floor_x
    frac_y = pos_y - floor_y
    frac_z = pos_z - floor_z
    cell_x = route[:, 0:1] * CX + floor_x.astype(jnp.int32)
    cell_y = floor_y.astype(jnp.int32)
    cell_z = floor_z.astype(jnp.int32)
    flat_grid = grid.reshape(NX * NY * NZ, CH)
    total = jnp.zeros(local_x.shape + (CH,), jnp.float32)
    for corner in range(8):
        step_x, step_y, step_z = corner // 4, (corner // 2) % 2, corner % 2
        factor = (frac_x if step_x else 1.0 - frac_x) * (frac_y if step_y else 1.0 - frac_y) * (frac_z if step_z else 1.0 - frac_z)
        index = ((cell_x + step_x) * NY + cell_y + step_y) * NZ + cell_z + step_z
        values = jnp.take(flat_grid, index, axis=0).astype(jnp.float32)
        total = total + factor[:, :, None] * values
    return jnp.sum(jnp.sum(total * weights, axis=2), axis=1)
```

```python
import jax
import jax.numpy as jnp
from jax import lax
from jax.experimental import pallas as pl
from jax.experimental.pallas import tpu as pltpu
from jax.sharding import PartitionSpec as P

SPAN = 32
SLOTS = 2
YB = 16
ZB = 16
LIVE_LANES = 120
DEAD = 99.0
BIG = 1.0e6


def smem():
    return pl.BlockSpec(memory_space=pltpu.SMEM)


def vmem():
    return pl.BlockSpec(memory_space=pltpu.VMEM)


def hbm():
    return pl.BlockSpec(memory_space=pl.ANY)


def send_kernel(tile, route, counts, base_y, base_z, types, offsets, out, spot, used, *, span_x):
    poses, atoms = types.shape
    slabs = out.shape[0]
    out[...] = jnp.zeros(out.shape, jnp.float32)

    def clear(i, carry):
        used[i] = 0
        return carry

    lax.fori_loop(0, slabs, clear, 0)
    lane = lax.broadcasted_iota(jnp.int32, (1, atoms), 1)
    row = lax.broadcasted_iota(jnp.int32, (8, atoms), 0)
    first = tile[0] * poses
    for p in range(poses):
        slab = route[first + p, 0]
        slot = used[slab]
        used[slab] = slot + 1
        spot[p] = SLOTS * slab + slot
        off = offsets[p]
        x = off[0:1] * span_x
        y = base_y[p].astype(jnp.float32) + off[1:2] * SPAN
        z = base_z[p].astype(jnp.float32) + off[2:3] * SPAN
        kind = jnp.where(lane < counts[p], types[p : p + 1].astype(jnp.float32), DEAD)
        kind = jnp.where(lane == LIVE_LANES, 1.0, kind)
        kind = jnp.where(lane == LIVE_LANES + 1, (base_y[p] // YB).astype(jnp.float32), kind)
        kind = jnp.where(lane == LIVE_LANES + 2, (base_z[p] // ZB).astype(jnp.float32), kind)
        block = jnp.concatenate([x, y, z, kind, x, y, z, kind], axis=0)
        out[slab] = jnp.where(row // 4 == slot, block, out[slab])


def hat(distance):
    return jnp.maximum(1.0 - jnp.abs(distance), 0.0)


def score_pose(key, incoming, table, cells, sums):
    slabs = incoming.shape[0]
    number = key // 128
    code = key % 128
    block_y = code // 8
    block_z = code % 8
    slab = number % slabs
    slot = number // slabs
    data = incoming[slab]
    data = jnp.where(slot == 0, data[0:4], data[4:8])
    shape = (8, data.shape[1])
    x = data[0:1]
    y = data[1:2] - (block_y * YB).astype(jnp.float32)
    z = jnp.broadcast_to(data[2:3] - (block_z * ZB).astype(jnp.float32), shape)
    lane = lax.broadcasted_iota(jnp.int32, (1, shape[1]), 1)
    kind = jnp.broadcast_to(jnp.where(lane < LIVE_LANES, data[3:4], DEAD), shape)
    coef = jnp.zeros(shape, jnp.float32)
    for t in range(table.shape[0]):
        coef = jnp.where(kind == t, table[t], coef)
    high, low = [], []
    for pair in range(3 * ZB // 2):
        parts = [hat(z - (2.0 * pair + i)) * coef for i in range(2)]
        part = jnp.concatenate(parts, axis=0)
        top = part.astype(jnp.bfloat16)
        high.append(top)
        low.append((part - top.astype(jnp.float32)).astype(jnp.bfloat16))
    right = jnp.concatenate(
        [jnp.concatenate(high, axis=0), jnp.concatenate(low, axis=0)], axis=1
    )
    rows = pl.ds(pl.multiple_of(block_y * YB, YB), 3 * YB)
    lanes = pl.ds(pl.multiple_of(block_z * 128, 128), 3 * 128)
    window = cells[:, rows, lanes].reshape(cells.shape[0] * 3 * YB, 3 * 128)
    mixed = jnp.dot(window, right, preferred_element_type=jnp.float32)
    total = jnp.zeros((3 * YB, shape[1]), jnp.float32)
    for i in range(cells.shape[0]):
        part = mixed[i * 3 * YB : (i + 1) * 3 * YB]
        total = total + hat(x - float(i)) * (part[:, : shape[1]] + part[:, shape[1] :])
    level = lax.broadcasted_iota(jnp.int32, total.shape, 0).astype(jnp.float32)
    total = total * hat(y - level)
    out = total[0:8]
    for i in range(1, 3 * YB // 8):
        out = out + total[8 * i : 8 * i + 8]
    sums[number] = out


def score_kernel(tile, incoming, weights, own, left, right, far_a, far_b, out, cells, table, sums, sems):
    tiles = cells.shape[1] // own.shape[1]
    height = own.shape[1]
    half = own.shape[0] // 2
    me = tile[0]

    def place(shift):
        return pl.ds(pl.multiple_of(lax.rem(me + shift, tiles) * height, height), height)

    copies = [
        pltpu.make_async_copy(own, cells.at[:, place(0), :], sems.at[0]),
        pltpu.make_async_copy(left, cells.at[:, place(tiles - 1), :], sems.at[1]),
        pltpu.make_async_copy(right, cells.at[:, place(1), :], sems.at[2]),
        pltpu.make_async_copy(far_a, cells.at[:half, place(2), :], sems.at[3]),
        pltpu.make_async_copy(far_b, cells.at[half:, place(2), :], sems.at[4]),
    ]
    for copy in copies:
        copy.start()
    slabs = incoming.shape[0]
    chans = weights.shape[1]
    atoms = incoming.shape[2]
    spread = jnp.transpose(weights[...])
    for t in range(weights.shape[0]):
        table[t] = jnp.broadcast_to(spread[:, t : t + 1], (chans, atoms))
    sums[...] = jnp.zeros(sums.shape, jnp.float32)
    heads = jnp.concatenate([incoming[:, 3, :], incoming[:, 7, :]], axis=0)
    heads = jnp.transpose(heads)[LIVE_LANES : LIVE_LANES + 8]
    number = lax.broadcasted_iota(jnp.int32, (1, SLOTS * slabs), 1).astype(jnp.float32)
    keys = number * 128.0 + heads[1:2] * 8.0 + heads[2:3]
    keys = jnp.where(heads[0:1] > 0.5, keys, BIG)
    count = jnp.sum(heads[0:1]).astype(jnp.int32)
    spare = float(SLOTS * slabs * 128)

    def draw(keys):
        least = jnp.min(keys)
        keys = jnp.where(keys == least, BIG, keys)
        return keys, jnp.minimum(least, spare).astype(jnp.int32)

    keys, one = draw(keys)
    keys, two = draw(keys)
    for copy in copies:
        copy.wait()

    def step(i, carry):
        keys, one, two = carry
        keys, next_one = draw(keys)
        keys, next_two = draw(keys)
        score_pose(one, incoming, table, cells, sums)
        score_pose(two, incoming, table, cells, sums)
        return keys, next_one, next_two

    lax.fori_loop(0, (count + 1) // 2, step, (keys, one, two))
    lane = lax.broadcasted_iota(jnp.int32, (slabs, atoms), 1)
    result = jnp.zeros((slabs, atoms), jnp.float32)
    for slot in range(SLOTS):
        part = jnp.sum(sums[slot * slabs : (slot + 1) * slabs], axis=1)
        part = jnp.sum(part, axis=1, keepdims=True)
        result = jnp.where(lane == slot, part, result)
    out[...] = result


def scored(grid, type_table, counts, types, offsets, route, base_y, base_z):
    slabs = lax.axis_size("slab")
    tiles = lax.axis_size("tile")
    cells_x, cells_y, wide_z = grid.shape
    poses, atoms = types.shape
    chans = type_table.shape[1]
    half = cells_x // 2
    up = [(i, (i + 1) % tiles) for i in range(tiles)]
    down = [(i, (i - 1) % tiles) for i in range(tiles)]
    left = lax.ppermute(grid, "tile", up)
    right = lax.ppermute(grid, "tile", down)
    far_a = lax.ppermute(left[:half], "tile", up)
    far_b = lax.ppermute(right[half:], "tile", down)
    tile = lax.axis_index("tile").astype(jnp.int32).reshape(1)
    outgoing, spot = pl.pallas_call(
        lambda *refs: send_kernel(*refs, span_x=float(cells_x - 1)),
        out_shape=(
            jax.ShapeDtypeStruct((slabs, 8, atoms), jnp.float32),
            jax.ShapeDtypeStruct((poses,), jnp.int32),
        ),
        in_specs=[smem(), smem(), smem(), smem(), smem(), vmem(), vmem()],
        out_specs=(vmem(), smem()),
        scratch_shapes=[pltpu.SMEM((slabs,), jnp.int32)],
        name="send",
    )(tile, route, counts, base_y, base_z, types, offsets)
    incoming = lax.all_to_all(outgoing, "slab", split_axis=0, concat_axis=0, tiled=True)
    partial = pl.pallas_call(
        score_kernel,
        out_shape=jax.ShapeDtypeStruct((slabs, atoms), jnp.float32),
        in_specs=[smem(), vmem(), vmem(), hbm(), hbm(), hbm(), hbm(), hbm()],
        out_specs=vmem(),
        scratch_shapes=[
            pltpu.VMEM((cells_x, tiles * cells_y, wide_z), jnp.bfloat16),
            pltpu.VMEM((type_table.shape[0], chans, atoms), jnp.float32),
            pltpu.VMEM((SLOTS * slabs + 1, 8, atoms), jnp.float32),
            pltpu.SemaphoreType.DMA((5,)),
        ],
        compiler_params=pltpu.CompilerParams(vmem_limit_bytes=32 << 20),
        cost_estimate=pl.CostEstimate(
            flops=4000000000, bytes_accessed=8 << 20, transcendentals=0
        ),
        name="score",
    )(tile, incoming, type_table, grid, left, right, far_a, far_b)
    returned = lax.all_to_all(partial, "slab", split_axis=0, concat_axis=0, tiled=True)
    flat = returned[:, :SLOTS].reshape(1, slabs * SLOTS)
    hits = spot[:, None] == jnp.arange(slabs * SLOTS, dtype=jnp.int32)[None, :]
    energy = jnp.sum(jnp.where(hits, flat, 0.0), axis=1)
    return energy / counts.astype(jnp.float32)


def solution(mesh):
    in_specs = (
        P("slab", "tile", None),
        P(),
        P(("slab", "tile")),
        P(("slab", "tile"), None),
        P(("slab", "tile"), None, None),
        P("slab", None),
        P(("slab", "tile")),
        P(("slab", "tile")),
    )
    out_specs = P(("slab", "tile"))
    return jax.shard_map(scored, mesh=mesh, in_specs=in_specs, out_specs=out_specs, check_vma=False)
```

```python
import functools
import jax
import jax.numpy as jnp
from jax import lax
from jax.experimental import pallas as pl
from jax.experimental.pallas import tpu as pltpu
from jax.sharding import PartitionSpec as P

SPAN = 32
SLOTS = 2
YB = 16
ZB = 16
NB = 3
LIVE_LANES = 120
DEAD = 99.0
BIG = 1.0e6


def smem():
    return pl.BlockSpec(memory_space=pltpu.SMEM)


def vmem():
    return pl.BlockSpec(memory_space=pltpu.VMEM)


def hbm():
    return pl.BlockSpec(memory_space=pl.ANY)


def send_kernel(tile, route, counts, base_y, base_z, types, offsets, out, pick, used, *, span_x):
    poses, atoms = types.shape
    slabs = out.shape[0]
    out[...] = jnp.zeros(out.shape, jnp.float32)

    def clear(i, carry):
        used[i] = 0
        return carry

    lax.fori_loop(0, slabs, clear, 0)
    lane = lax.broadcasted_iota(jnp.int32, (1, atoms), 1)
    row = lax.broadcasted_iota(jnp.int32, (8, atoms), 0)
    first = tile[0] * poses
    for p in range(poses):
        slab = route[first + p]
        slot = used[slab]
        used[slab] = slot + 1
        count = jnp.broadcast_to(counts[p].astype(jnp.float32), (1, atoms))
        pick[p : p + 1] = jnp.where(lane == SLOTS * slab + slot, 1.0 / count, 0.0)
        x = offsets[0, p : p + 1] * span_x
        y = base_y[p].astype(jnp.float32) + offsets[1, p : p + 1] * SPAN
        z = base_z[p].astype(jnp.float32) + offsets[2, p : p + 1] * SPAN
        kind = jnp.where(lane < counts[p], types[p : p + 1].astype(jnp.float32), DEAD)
        kind = jnp.where(lane == LIVE_LANES, 1.0, kind)
        kind = jnp.where(lane == LIVE_LANES + 1, (base_y[p] // YB).astype(jnp.float32), kind)
        kind = jnp.where(lane == LIVE_LANES + 2, (base_z[p] // ZB).astype(jnp.float32), kind)
        block = jnp.concatenate([x, y, z, kind, x, y, z, kind], axis=0)
        out[slab] = jnp.where(row // 4 == slot, block, out[slab])


def hat(distance):
    return jnp.maximum(1.0 - jnp.abs(distance), 0.0)


def split_key(key, slabs):
    number = key // 128
    code = key % 128
    return number, number % slabs, number // slabs, code // 8, code % 8


def build(key, incoming, table, hats, right):
    _, slab, slot, _, block_z = split_key(key, incoming.shape[0])
    data = incoming[slab]
    data = jnp.where(slot == 0, data[0:4], data[4:8])
    atoms = data.shape[1]
    lane = lax.broadcasted_iota(jnp.int32, (1, atoms), 1)
    level = lax.broadcasted_iota(jnp.int32, (NB * ZB, atoms), 0).astype(jnp.float32)
    hats[...] = hat(data[2:3] - (block_z * ZB).astype(jnp.float32) - level)
    shape = (table.shape[1], atoms)
    kind = jnp.broadcast_to(jnp.where(lane < LIVE_LANES, data[3:4], DEAD), shape)
    coef = jnp.zeros(shape, jnp.float32)
    for t in range(table.shape[0]):
        coef = jnp.where(kind == t, table[t], coef)
    for pair in range(NB * ZB // 2):
        parts = [
            jnp.broadcast_to(hats[2 * pair + i : 2 * pair + i + 1], shape) * coef
            for i in range(2)
        ]
        part = jnp.concatenate(parts, axis=0)
        top = part.astype(jnp.bfloat16)
        rows = slice(2 * pair * shape[0], 2 * (pair + 1) * shape[0])
        right[rows, :atoms] = top
        right[rows, atoms:] = (part - top.astype(jnp.float32)).astype(jnp.bfloat16)


def apply(key, incoming, window, start_y, right, hats, sums):
    number, slab, slot, _, _ = split_key(key, incoming.shape[0])
    data = incoming[slab]
    data = jnp.where(slot == 0, data[0:4], data[4:8])
    atoms = data.shape[1]
    wide = window.shape[0]
    mixed = jnp.dot(
        window.reshape(wide * NB * YB, window.shape[2]),
        right[...],
        preferred_element_type=jnp.float32,
    )
    level = lax.broadcasted_iota(jnp.int32, (wide, atoms), 0).astype(jnp.float32)
    hats[...] = hat(data[0:1] - level)
    total = None
    for i in range(wide):
        part = mixed[i * NB * YB : (i + 1) * NB * YB]
        part = hats[i : i + 1] * (part[:, :atoms] + part[:, atoms:])
        total = part if total is None else total + part
    level = lax.broadcasted_iota(jnp.int32, total.shape, 0).astype(jnp.float32)
    total = total * hat(data[1:2] - start_y.astype(jnp.float32) - level)
    out = total[0:8]
    for i in range(1, NB * YB // 8):
        out = out + total[8 * i : 8 * i + 8]
    sums[number] = out


def score(incoming, weights, wanted, window_of, table, sums, tools):
    slabs, _, atoms = incoming.shape
    z_hats, x_hats, rights = tools
    chans = weights.shape[0]
    for t in range(weights.shape[1]):
        table[t] = jnp.broadcast_to(weights[:, t : t + 1], (chans, atoms))
    sums[...] = jnp.zeros(sums.shape, jnp.float32)
    heads = jnp.concatenate([incoming[:, 3, :], incoming[:, 7, :]], axis=0)
    heads = jnp.transpose(heads)[LIVE_LANES : LIVE_LANES + 8]
    number = lax.broadcasted_iota(jnp.int32, (1, SLOTS * slabs), 1).astype(jnp.float32)
    keys = number * 128.0 + heads[1:2] * 8.0 + heads[2:3]
    live = (heads[0:1] > 0.5) & wanted(heads[1:2])
    keys = jnp.where(live, keys, BIG)
    count = jnp.sum(jnp.where(live, 1.0, 0.0)).astype(jnp.int32)
    spare = float(SLOTS * slabs * 128)

    def draw(keys):
        least = jnp.min(keys)
        keys = jnp.where(keys == least, BIG, keys)
        return keys, jnp.minimum(least, spare).astype(jnp.int32)

    def put(key, i):
        build(key, incoming, table, z_hats[i], rights[i])

    def use(key, i):
        _, _, _, block_y, block_z = split_key(key, slabs)
        lanes = pl.ds(pl.multiple_of(block_z * 128, 128), NB * 128)
        window, start_y = window_of(block_y, lanes)
        apply(key, incoming, window, start_y, rights[i], x_hats[i], sums)

    keys, one = draw(keys)
    keys, two = draw(keys)
    put(one, 0)

    def step(i, carry):
        keys, one, two = carry
        keys, three = draw(keys)
        keys, four = draw(keys)
        use(one, 0)
        put(two, 1)
        use(two, 1)
        put(three, 0)
        return keys, three, four

    lax.fori_loop(0, (count + 1) // 2, step, (keys, one, two))
    lane = lax.broadcasted_iota(jnp.int32, (slabs, atoms), 1)
    result = jnp.zeros((slabs, atoms), jnp.float32)
    for slot in range(SLOTS):
        part = jnp.sum(sums[slot * slabs : (slot + 1) * slabs], axis=1)
        part = jnp.sum(part, axis=1, keepdims=True)
        result = jnp.where(lane == slot, part, result)
    return result


def tile_of(block, per_tile):
    return jnp.floor((block + 0.5) / per_tile)


def near_kernel(tile, incoming, weights, own, left_a, left_b, right_a, right_b, out, cells, sems, table, sums, *tools):
    height = own.shape[1]
    tiles = cells.shape[1] // height
    half = left_a.shape[0]
    me = tile[0]

    def place(shift):
        return pl.ds(pl.multiple_of(lax.rem(me + shift, tiles) * height, height), height)

    copies = [
        pltpu.make_async_copy(own, cells.at[:, place(0), :], sems.at[0]),
        pltpu.make_async_copy(left_a, cells.at[:half, place(tiles - 1), :], sems.at[1]),
        pltpu.make_async_copy(left_b, cells.at[half:, place(tiles - 1), :], sems.at[2]),
        pltpu.make_async_copy(right_a, cells.at[:half, place(1), :], sems.at[3]),
        pltpu.make_async_copy(right_b, cells.at[half:, place(1), :], sems.at[4]),
    ]
    for copy in copies:
        copy.start()
    cells[:, place(2), :] = jnp.zeros(own.shape, cells.dtype)
    far = lax.rem(me + 2, tiles).astype(jnp.float32)
    for copy in copies:
        copy.wait()

    def wanted(block):
        per = height // YB
        return (tile_of(block, per) != far) | (tile_of(block + (NB - 1), per) != far)

    def window_of(block, lanes):
        start = block * YB
        return cells[:, pl.ds(pl.multiple_of(start, YB), NB * YB), lanes], start

    out[...] = score(incoming, weights, wanted, window_of, table, sums, (tools[0:2], tools[2:4], tools[4:6]))


def far_kernel(tile, incoming, weights, near, far_a, far_b, out, table, sums, *tools, tiles):
    height = far_a.shape[1]
    per = height // YB
    far = lax.rem(tile[0] + 2, tiles)
    far_f = far.astype(jnp.float32)

    def wanted(block):
        return (tile_of(block, per) == far_f) | (tile_of(block + (NB - 1), per) == far_f)

    def window_of(block, lanes):
        start = jnp.clip(block - per * far, 0, per - NB) * YB
        rows = pl.ds(pl.multiple_of(start, YB), NB * YB)
        window = jnp.concatenate([far_a[:, rows, lanes], far_b[:, rows, lanes]], axis=0)
        return window, start + far * height

    more = score(incoming, weights, wanted, window_of, table, sums, (tools[0:2], tools[2:4], tools[4:6]))
    out[...] = near[...] + more


def scored(grid, type_table, counts, types, offsets, route, base_y, base_z):
    slabs = lax.axis_size("slab")
    tiles = lax.axis_size("tile")
    cells_x, cells_y, wide_z = grid.shape
    poses, atoms = types.shape
    kinds, chans = type_table.shape
    half = cells_x // 2
    up = [(i, (i + 1) % tiles) for i in range(tiles)]
    down = [(i, (i - 1) % tiles) for i in range(tiles)]
    left_a = lax.ppermute(grid[:half], "tile", up)
    right_b = lax.ppermute(grid[half:], "tile", down)
    left_b = lax.ppermute(grid[half:], "tile", up)
    right_a = lax.ppermute(grid[:half], "tile", down)
    far_a = lax.ppermute(left_a, "tile", up)
    far_b = lax.ppermute(right_b, "tile", down)
    tile = lax.axis_index("tile").astype(jnp.int32).reshape(1)
    outgoing, pick = pl.pallas_call(
        functools.partial(send_kernel, span_x=float(cells_x - 1)),
        out_shape=(
            jax.ShapeDtypeStruct((slabs, 8, atoms), jnp.float32),
            jax.ShapeDtypeStruct((poses, atoms), jnp.float32),
        ),
        in_specs=[smem(), smem(), smem(), smem(), smem(), vmem(), vmem()],
        out_specs=(vmem(), vmem()),
        scratch_shapes=[pltpu.SMEM((slabs,), jnp.int32)],
        name="send",
    )(tile, route.reshape(-1), counts, base_y, base_z, types, jnp.swapaxes(offsets, 0, 1))
    incoming = lax.all_to_all(outgoing, "slab", split_axis=0, concat_axis=0, tiled=True)
    weights = jnp.swapaxes(type_table, 0, 1)
    result = jax.ShapeDtypeStruct((slabs, atoms), jnp.float32)
    shared = [
        pltpu.VMEM((kinds, chans, atoms), jnp.float32),
        pltpu.VMEM((SLOTS * slabs + 1, 8, atoms), jnp.float32),
        pltpu.VMEM((NB * ZB, atoms), jnp.float32),
        pltpu.VMEM((NB * ZB, atoms), jnp.float32),
        pltpu.VMEM((cells_x, atoms), jnp.float32),
        pltpu.VMEM((cells_x, atoms), jnp.float32),
        pltpu.VMEM((NB * ZB * chans, 2 * atoms), jnp.bfloat16),
        pltpu.VMEM((NB * ZB * chans, 2 * atoms), jnp.bfloat16),
    ]
    near = pl.pallas_call(
        near_kernel,
        out_shape=result,
        in_specs=[smem(), vmem(), vmem()] + [hbm()] * 5,
        out_specs=vmem(),
        scratch_shapes=[
            pltpu.VMEM((cells_x, tiles * cells_y, wide_z), jnp.bfloat16),
            pltpu.SemaphoreType.DMA((5,)),
        ]
        + shared,
        compiler_params=pltpu.CompilerParams(vmem_limit_bytes=32 << 20),
        cost_estimate=pl.CostEstimate(
            flops=4000000000, bytes_accessed=6 << 20, transcendentals=0
        ),
        name="near",
    )(tile, incoming, weights, grid, left_a, left_b, right_a, right_b)
    partial = pl.pallas_call(
        functools.partial(far_kernel, tiles=tiles),
        out_shape=result,
        in_specs=[smem()] + [vmem()] * 5,
        out_specs=vmem(),
        scratch_shapes=shared,
        compiler_params=pltpu.CompilerParams(vmem_limit_bytes=32 << 20),
        cost_estimate=pl.CostEstimate(
            flops=1000000000, bytes_accessed=2 << 20, transcendentals=0
        ),
        name="far",
    )(tile, incoming, weights, near, far_a, far_b)
    returned = lax.all_to_all(partial, "slab", split_axis=0, concat_axis=0, tiled=True)
    flat = returned[:, :SLOTS].reshape(1, slabs * SLOTS)
    return jnp.sum(flat * pick, axis=1)


def solution(mesh):
    in_specs = (
        P("slab", "tile", None),
        P(),
        P(("slab", "tile")),
        P(("slab", "tile"), None),
        P(("slab", "tile"), None, None),
        P("slab", None),
        P(("slab", "tile")),
        P(("slab", "tile")),
    )
    out_specs = P(("slab", "tile"))
    return jax.shard_map(scored, mesh=mesh, in_specs=in_specs, out_specs=out_specs, check_vma=False)
```
